32 devices in a mesh: dp: 8 (over z, y), mp: 2 (over core), fsdp: 2 (over x).
Axes of the slice: x: 2, y: 2, z: 4, core: 2. Of those that a mesh axis runs over, the one named last changes fastest.
Arguments:
- features: bfloat16 [5, 1024, 512], P(None, ('dp', 'fsdp')), may hold values from -6 to 6
- memory_bank: bfloat16 [512, 32, 1024], P(('dp', 'fsdp')), may hold values from -1 to 1
- memory_fill: int32 [512], P(('dp', 'fsdp')), may hold values from 0 to 32
- left_keys: bfloat16 [512, 64, 1024], P(('dp', 'fsdp'), None, 'mp'), may hold values from -400 to 400
- left_values: bfloat16 [512, 64, 1024], P(('dp', 'fsdp'), None, 'mp'), may hold values from -6 to 6
- left_length: int32 [512], P(('dp', 'fsdp')), may hold values from 0 to 64
- w_query: bfloat16 [1024, 1024], P('fsdp', 'mp'), may hold values from -0.1875 to 0.1875
- w_key: bfloat16 [1024, 1024], P('fsdp', 'mp'), may hold values from -0.1875 to 0.1875
- w_value: bfloat16 [1024, 1024], P('fsdp', 'mp'), may hold values from -0.1875 to 0.1875
- w_out: bfloat16 [1024, 1024], P('mp', 'fsdp'), may hold values from -0.1875 to 0.1875
- w_up: bfloat16 [1024, 4096], P('fsdp', 'mp'), may hold values from -0.1875 to 0.1875
- w_down: bfloat16 [4096, 1024], P('mp', 'fsdp'), may hold values from -0.09375 to 0.09375
- out_gain: float32 [1024], replicated, may hold values from 0.1 to 1.9
Outputs:
- layer_out: bfloat16 [512, 5, 1024], P(('dp', 'fsdp'))
- memory_next: bfloat16 [512, 1024], P(('dp', 'fsdp'))
- center_keys: bfloat16 [512, 4, 1024], P(('dp', 'fsdp'), None, 'mp')
- center_values: bfloat16 [512, 4, 1024], P(('dp', 'fsdp'), None, 'mp')
The draws below stay inside these ranges and needn't reach their ends.
All inputs are finite; a program needn't handle non-finite values.
Results may differ from the reference program's by a relative error of at most 0.0095.
Values may be sent and summed in bfloat16 or wider, within the bound.
A program may use at most 128 MiB of HBM per device.

```python
import jax
import jax.numpy as jnp
from jax import lax

D = 1024
H = 16
HD = 64
FF = 4096
MEM = 32
LEFT = 64
GROUP = 4
FRAMES = 5
STR_DEV = 32
STREAMS = 512


def draw_left_keys(key, part):
    base = jnp.clip(jax.random.normal(jax.random.fold_in(key, 11), (STREAMS, LEFT, D), jnp.float32), -6.0, 6.0)
    return base.astype(jnp.bfloat16)


def set_ends(entries, key, least, top_value):
    place = [jax.random.randint(jax.random.fold_in(key, axis), (), 0, length) for axis, length in enumerate(entries.shape)]
    main_axis = entries.shape.index(max(entries.shape))
    beside = place[:main_axis] + [(place[main_axis] + 1) % entries.shape[main_axis]] + place[main_axis + 1:]
    return entries.at[tuple(place)].set(least).at[tuple(beside)].set(top_value)


def raised(values, key, source, target, parts, factor):
    def block_of(dim):
        return (jnp.arange(values.shape[dim]) // (values.shape[dim] // parts)).reshape((-1,) + (1,) * (values.ndim - 1 - dim))

    one_side = jax.random.permutation(key, parts)[block_of(target)]
    second = (block_of(target) + parts // 2) % parts
    return jnp.where((block_of(source) == one_side) | (block_of(source) == second), factor * values, values)


def levels(own_key, extent, pieces, smallest, top_value):
    level = 1.0
    for position, shards_of in pieces:
        heights = jax.random.uniform(jax.random.fold_in(jax.random.fold_in(own_key, 6), position), (shards_of,), jnp.float32, smallest / len(pieces), top_value / len(pieces))
        level = level * jnp.repeat(jnp.exp(heights), extent[position] // shards_of).reshape((-1,) + (1,) * (len(extent) - 1 - position))
    return level


def normal_values(stream_key, dims, width, most, shards=(), held_as=jnp.bfloat16):
    values = jax.random.normal(stream_key, dims, jnp.float32) * width
    if len(shards) > 0:
        values = levels(stream_key, dims, shards, -0.22, 0.18) * values
    return jnp.clip(values, min=-most, max=most).astype(held_as)


def bell_draw_with(stream_key, shape, width, limit, cuts, heavy, kind=jnp.bfloat16):
    values = width * jax.random.normal(stream_key, shape, jnp.float32)
    if cuts:
        values = values * levels(stream_key, shape, cuts, -0.22, 0.18)
    return jnp.clip(raised(values, jax.random.fold_in(stream_key, 3), *heavy), -limit, limit).astype(kind)


def setup_inputs(seed: int = 0) -> dict:
    streams_of = jax.random.split(jax.random.key(seed), 14)
    features = bell_draw_with(streams_of[0], (FRAMES, D, STREAMS), 1.0, 6.0, ((1, 16),), (1, 2, 16, 2.0))
    memory_bank = jnp.clip(jax.random.uniform(streams_of[1], (STREAMS, MEM, D), jnp.float32, -1.0, 1.0) * levels(streams_of[1], (STREAMS, MEM, D), ((0, 16),), -0.4, 0.0), -1.0, 1.0).astype(jnp.bfloat16)
    memory_fill = set_ends(jax.random.randint(streams_of[2], (STREAMS,), 0, MEM + 1), jax.random.fold_in(streams_of[2], 1), 0, MEM).astype(jnp.int32)
    left_keys = draw_left_keys(jax.random.fold_in(streams_of[13], 71), 0)
    left_values = normal_values(streams_of[4], (STREAMS, LEFT, D), 1.0, 6.0, ((0, 16), (2, 2)))
    left_length = set_ends(jax.random.randint(streams_of[5], (STREAMS,), 0, LEFT + 1), jax.random.fold_in(streams_of[5], 1), 0, LEFT).astype(jnp.int32)
    w_query = normal_values(streams_of[6], (D, D), D ** -0.5, 0.1875, ((0, 2), (1, 2)))
    w_key = normal_values(streams_of[7], (D, D), D ** -0.5, 0.1875, ((0, 2), (1, 2)))
    w_value = normal_values(streams_of[8], (D, D), D ** -0.5, 0.1875, ((0, 2), (1, 2)))
    w_out = normal_values(streams_of[9], (D, D), D ** -0.5, 0.1875, ((0, 2), (1, 2)))
    w_up = normal_values(streams_of[10], (D, FF), D ** -0.5, 0.1875, ((0, 2), (1, 2)))
    w_down = normal_values(streams_of[11], (FF, D), FF ** -0.5, 0.09375, ((0, 2), (1, 2)))
    out_gain = jnp.clip(1.0 + 0.18 * jax.random.normal(streams_of[12], (D,), jnp.float32), 0.1, 1.9)
    return {"features": features, "memory_bank": memory_bank, "memory_fill": memory_fill, "left_keys": left_keys, "left_values": left_values, "left_length": left_length, "w_query": w_query, "w_key": w_key, "w_value": w_value, "w_out": w_out, "w_up": w_up, "w_down": w_down, "out_gain": out_gain}


epsilon = 1e-05
masked_score = -1e+30

def normalize(values):
    values = values.astype(jnp.float32)
    average = lax.optimization_barrier(jnp.mean(values, axis=-1, keepdims=True))
    centred = values - average
    variance = lax.optimization_barrier(jnp.mean(centred * centred, axis=-1, keepdims=True))
    return centred * lax.rsqrt(variance + epsilon)

def visible_masks(fill, length, mem_slots, left_slots, query_count):
    mem_ok = jnp.arange(mem_slots, dtype=jnp.int32)[None, :] >= (mem_slots - fill)[:, None]
    not_summary = jnp.arange(query_count, dtype=jnp.int32) < query_count - 1
    mem_mask = mem_ok[:, None, None, :] & not_summary[None, None, :, None]
    left_ok = jnp.arange(left_slots, dtype=jnp.int32)[None, :] >= (left_slots - length)[:, None]
    left_mask = left_ok[:, None, None, :] & (not_summary[None, None, :, None] | True)
    return (mem_mask, left_mask)

def reference(features, memory_bank, memory_fill, left_keys, left_values, left_length, w_query, w_key, w_value, w_out, w_up, w_down, out_gain):
    streams = features.shape[2]
    inputs = jnp.transpose(features, (2, 0, 1))
    normed = normalize(inputs).astype(jnp.bfloat16)
    summary = lax.optimization_barrier(jnp.mean(normed[:, :GROUP, :].astype(jnp.float32), axis=1)).astype(jnp.bfloat16)
    query_rows = jnp.concatenate([normed, summary[:, None, :]], axis=1).reshape(-1, D)
    query_proj = jnp.dot(query_rows, w_query, preferred_element_type=jnp.float32).astype(jnp.bfloat16)
    group_rows = normed.reshape(-1, D)
    group_keys = jnp.dot(group_rows, w_key, preferred_element_type=jnp.float32).astype(jnp.bfloat16)
    group_values = jnp.dot(group_rows, w_value, preferred_element_type=jnp.float32).astype(jnp.bfloat16)
    blocks = streams // STR_DEV
    scale = HD ** (-0.5)

    def split(array):
        return array.reshape((blocks, STR_DEV) + array.shape[1:])

    def attend(operands):
        query_blk, ckey_blk, cval_blk, memory_blk, lkey_blk, lval_blk, fill_blk, length_blk = operands
        memory_rows = memory_blk.reshape(-1, D)
        mem_keys = jnp.dot(memory_rows, w_key, preferred_element_type=jnp.float32).astype(jnp.bfloat16)
        mem_values = jnp.dot(memory_rows, w_value, preferred_element_type=jnp.float32).astype(jnp.bfloat16)
        query_h = query_blk.reshape(STR_DEV, FRAMES + 1, H, HD).astype(jnp.float32)
        mkey_h = mem_keys.reshape(STR_DEV, MEM, H, HD).astype(jnp.float32)
        mval_h = mem_values.reshape(STR_DEV, MEM, H, HD).astype(jnp.float32)
        lkey_h = lkey_blk.reshape(STR_DEV, LEFT, H, HD).astype(jnp.float32)
        lval_h = lval_blk.reshape(STR_DEV, LEFT, H, HD).astype(jnp.float32)
        ckey_h = ckey_blk.reshape(STR_DEV, FRAMES, H, HD).astype(jnp.float32)
        cval_h = cval_blk.reshape(STR_DEV, FRAMES, H, HD).astype(jnp.float32)
        mem_mask, left_mask = visible_masks(fill_blk, length_blk, MEM, LEFT, FRAMES + 1)
        score_mem = jnp.einsum('sqhd,skhd->shqk', query_h, mkey_h) * scale
        score_left = jnp.einsum('sqhd,skhd->shqk', query_h, lkey_h) * scale
        score_group = jnp.einsum('sqhd,skhd->shqk', query_h, ckey_h) * scale
        score_mem = jnp.where(mem_mask, score_mem, masked_score)
        score_left = jnp.where(left_mask, score_left, masked_score)
        top = jnp.maximum(jnp.maximum(lax.optimization_barrier(jnp.max(score_mem, axis=-1, keepdims=True)), lax.optimization_barrier(jnp.max(score_left, axis=-1, keepdims=True))), lax.optimization_barrier(jnp.max(score_group, axis=-1, keepdims=True)))
        exp_mem = jnp.exp(score_mem - top)
        exp_left = jnp.exp(score_left - top)
        exp_group = jnp.exp(score_group - top)
        totals = lax.optimization_barrier(jnp.sum(exp_mem, axis=-1, keepdims=True)) + lax.optimization_barrier(jnp.sum(exp_left, axis=-1, keepdims=True)) + lax.optimization_barrier(jnp.sum(exp_group, axis=-1, keepdims=True))
        prob_mem = (exp_mem / totals).astype(jnp.bfloat16).astype(jnp.float32)
        prob_left = (exp_left / totals).astype(jnp.bfloat16).astype(jnp.float32)
        prob_group = (exp_group / totals).astype(jnp.bfloat16).astype(jnp.float32)
        attended = jnp.einsum('shqk,skhd->sqhd', prob_mem, mval_h) + jnp.einsum('shqk,skhd->sqhd', prob_left, lval_h) + jnp.einsum('shqk,skhd->sqhd', prob_group, cval_h)
        return attended.astype(jnp.bfloat16).reshape(STR_DEV, FRAMES + 1, D)
    attended = lax.map(attend, (split(query_proj.reshape(streams, (FRAMES + 1) * D)), split(group_keys.reshape(streams, FRAMES * D)), split(group_values.reshape(streams, FRAMES * D)), split(memory_bank), split(left_keys), split(left_values), split(memory_fill), split(left_length)))
    attended = attended.reshape(-1, D)
    attn_out = jnp.dot(attended, w_out, preferred_element_type=jnp.float32).reshape(streams, FRAMES + 1, D)
    memory_next = jnp.tanh(attn_out[:, FRAMES, :]).astype(jnp.bfloat16)
    hidden_state = inputs.astype(jnp.float32) + attn_out[:, :FRAMES, :]
    h_norm = normalize(hidden_state).astype(jnp.bfloat16).reshape(-1, D)
    up_proj = jax.nn.gelu(jnp.dot(h_norm, w_up, preferred_element_type=jnp.float32), approximate=True).astype(jnp.bfloat16)
    down_proj = jnp.dot(up_proj, w_down, preferred_element_type=jnp.float32)
    layer_out = (normalize(hidden_state.reshape(-1, D) + down_proj) * out_gain.astype(jnp.float32)).astype(jnp.bfloat16).reshape(streams, FRAMES, D)
    center_keys = group_keys.reshape(streams, FRAMES, D)[:, :GROUP, :]
    center_values = group_values.reshape(streams, FRAMES, D)[:, :GROUP, :]
    return (layer_out, memory_next, center_keys, center_values)
```

```python
import functools

import jax
import jax.numpy as jnp
from jax import lax
from jax.experimental import pallas as pl
from jax.experimental.pallas import tpu as pltpu
from jax.sharding import PartitionSpec as P

HD = 64
GROUP = 4
ROWS = 8
KEYS = 128

epsilon = 1e-05
masked_score = -1e30
MESH = pl.DeviceIdType.MESH
bf16 = jnp.bfloat16
f32 = jnp.float32


def normalize(values):
    average = jnp.mean(values, axis=-1, keepdims=True)
    centred = values - average
    variance = jnp.mean(centred * centred, axis=-1, keepdims=True)
    return centred * lax.rsqrt(variance + epsilon)


def matmul(left, right):
    return jnp.dot(left, right, preferred_element_type=f32)


def body(
    frames,
    mem_slots,
    left_slots,
    x_ref,
    bias_ref,
    gain_ref,
    mem_hbm,
    lk_hbm,
    lv_hbm,
    wq_hbm,
    wk_hbm,
    wv_hbm,
    wo_hbm,
    wu_hbm,
    wd_hbm,
    out_ref,
    mnext_ref,
    ck_ref,
    cv_ref,
    far,
    own,
    mem_v,
    lk_v,
    lv_v,
    mk,
    mv,
    gk,
    gv,
    qs,
    rows_v,
    att,
    hid,
    hbuf,
    dacc,
    part,
    peer,
    send_sem,
    recv_sem,
    psend_sem,
    precv_sem,
    load_sem,
):
    d = lax.axis_index("dp")
    m = lax.axis_index("mp")
    f = lax.axis_index("fsdp")
    total, width = x_ref.shape
    streams = total // ROWS
    n_blocks, depth, cols = far.shape
    n_ff = (n_blocks - 4) // 2
    quarter = depth // 4
    c1 = quarter // 4
    c2 = (quarter - c1) // 2
    ybit = lax.rem(d, 2)
    zbit = lax.rem(lax.div(d, 2), 2)
    p = lax.rem(d, 4)
    py = p + 1 - 2 * ybit
    pz = p + 2 - 4 * zbit
    pd = 3 - p
    xdev = (d, m, 1 - f)
    ydev = (d + 1 - 2 * ybit, m, f)
    zdev = (d + 2 - 4 * zbit, m, f)
    mdev = (d, 1 - m, f)

    def own_hbm(b, start, size):
        r = pl.ds(pl.multiple_of(start, 16), size)
        if b < 4:
            return (wk_hbm, wv_hbm, wq_hbm, wo_hbm)[b].at[r, :]
        j = (b - 4) // 2
        if b % 2 == 0:
            return wu_hbm.at[r, pl.ds(j * cols, cols)]
        return wd_hbm.at[pl.ds(pl.multiple_of(start + j * depth, 16), size), :]

    def piece(b, start, size):
        return far.at[b, pl.ds(pl.multiple_of(start, 16), size), :]

    sends = []

    def send(src, b, start, size, dev, kind):
        copy = pltpu.make_async_remote_copy(
            src_ref=src,
            dst_ref=piece(b, start, size),
            send_sem=send_sem.at[b, kind],
            recv_sem=recv_sem.at[b, kind],
            device_id=dev,
            device_id_type=MESH,
        )
        copy.start()
        sends.append(copy)

    def arrived(b, start, size, kind):
        ref = piece(b, start, size)
        pltpu.make_async_remote_copy(
            src_ref=ref,
            dst_ref=ref,
            send_sem=send_sem.at[b, kind],
            recv_sem=recv_sem.at[b, kind],
            device_id=xdev,
            device_id_type=MESH,
        ).wait_recv()

    def load(src, dst, i):
        copy = pltpu.make_async_copy(src, dst, load_sem.at[i])
        copy.start()
        return copy

    barrier = pltpu.get_barrier_semaphore()
    for dev in (xdev, ydev, zdev, mdev):
        pl.semaphore_signal(barrier, inc=1, device_id=dev, device_id_type=MESH)
    pl.semaphore_wait(barrier, 4)

    for b in range(n_blocks):
        send(own_hbm(b, p * quarter, quarter), b, p * quarter, quarter, xdev, 0)
        send(own_hbm(b, pd * quarter, c1), b, pd * quarter, c1, xdev, 1)

    loads = [load(own_hbm(b, 0, depth), own.at[b], b) for b in range(n_blocks)]
    mem_load = load(mem_hbm, mem_v, n_blocks)
    lk_load = load(lk_hbm, lk_v, n_blocks + 1)
    lv_load = load(lv_hbm, lv_v, n_blocks + 2)

    def pass_quarter(b):
        if b >= n_blocks:
            return
        arrived(b, p * quarter, quarter, 0)
        src = piece(b, p * quarter, quarter)
        send(src, b, p * quarter, quarter, ydev, 2)
        send(src, b, p * quarter, quarter, zdev, 3)

    def pass_diagonal(b):
        if b >= n_blocks:
            return
        at_y = pz * quarter + c1
        arrived(b, pz * quarter, quarter, 3)
        send(piece(b, at_y, c2), b, at_y, c2, ydev, 4)
        at_z = py * quarter + c1 + c2
        arrived(b, py * quarter, quarter, 2)
        send(piece(b, at_z, c2), b, at_z, c2, zdev, 5)

    def complete(b):
        arrived(b, pd * quarter, c1, 1)
        arrived(b, pd * quarter + c1, c2, 4)
        arrived(b, pd * quarter + c1 + c2, c2, 5)

    def pump(b):
        pass_quarter(b)
        pass_diagonal(b - 1)

    mine = pl.ds(pl.multiple_of(f * depth, 128), depth)
    other = pl.ds(pl.multiple_of((1 - f) * depth, 128), depth)
    tile = 64

    @pl.loop(0, total // tile)
    def _(i):
        r = pl.ds(pl.multiple_of(i * tile, tile), tile)
        n = normalize(x_ref[r, :].astype(f32)).astype(bf16).astype(f32)
        n3 = n.reshape(tile // ROWS, ROWS, width)
        row = lax.broadcasted_iota(jnp.int32, n3.shape, 1)
        mean = jnp.sum(jnp.where(row < GROUP, n3, 0.0), axis=1, keepdims=True) * (1.0 / GROUP)
        n3 = jnp.where(row == frames, jnp.broadcast_to(mean, n3.shape), n3)
        rows_v[r, :] = n3.reshape(tile, width).astype(bf16)

    mem_load.wait()
    pass_quarter(0)
    pump(1)

    def project(b):
        loads[b].wait()
        complete(b)
        sums = matmul(rows_v[:, mine], own[b]) + matmul(rows_v[:, other], far[b])
        return sums.astype(bf16)

    def project_memory(b, target):
        step = 256

        @pl.loop(0, mem_v.shape[0] // step)
        def _(i):
            r = pl.ds(pl.multiple_of(i * step, step), step)
            sums = matmul(mem_v[r, mine], own[b]) + matmul(mem_v[r, other], far[b])
            target[r, :] = sums.astype(bf16)

    keys = project(0)
    ck_ref[...] = keys
    gk[...] = keys.astype(f32)
    project_memory(0, mk)
    pump(2)
    vals = project(1)
    cv_ref[...] = vals
    gv[...] = vals.astype(f32)
    project_memory(1, mv)
    pump(3)
    qs[...] = project(2).astype(f32)
    lk_load.wait()
    lv_load.wait()

    heads = cols // HD
    lanes3 = lax.broadcasted_iota(jnp.int32, (heads, ROWS, cols), 2)
    head3 = lax.broadcasted_iota(jnp.int32, (heads, ROWS, cols), 0)
    head_mask = jnp.where(lanes3 // HD == head3, 1.0, 0.0).astype(f32)
    row2 = lax.broadcasted_iota(jnp.int32, (heads * ROWS, KEYS), 0)
    lane2 = lax.broadcasted_iota(jnp.int32, (heads * ROWS, KEYS), 1)
    excluded = jnp.where((row2 % ROWS == frames) & (lane2 < mem_slots), -1.0, 0.0).astype(f32)
    pad8 = jnp.zeros((16 - ROWS, cols), f32)
    pad = jnp.zeros((KEYS - mem_slots - left_slots - 16, cols), bf16)
    scale = HD ** (-0.5)

    def gather_rows(mem_part, left_part, group_part, s):
        return jnp.concatenate(
            [
                mem_part[pl.ds(pl.multiple_of(s * mem_slots, mem_slots), mem_slots), :],
                left_part[s],
                jnp.concatenate(
                    [group_part[pl.ds(pl.multiple_of(s * ROWS, ROWS), ROWS), :], pad8], axis=0
                ).astype(bf16),
                pad,
            ],
            axis=0,
        )

    def attend(s):
        r = pl.ds(pl.multiple_of(s * ROWS, ROWS), ROWS)
        spread = (qs[r, :][None] * head_mask).reshape(heads * ROWS, cols).astype(bf16)
        k = gather_rows(mk, lk_v, gk, s)
        scores = (
            lax.dot_general(spread, k, (((1,), (1,)), ((), ())), preferred_element_type=f32) * scale
        )
        hide = bias_ref[pl.ds(s, 1), :] + excluded
        scores = jnp.where(hide < 0.0, masked_score, scores)
        top = jnp.max(scores, axis=-1, keepdims=True)
        e = jnp.exp(scores - top)
        probs = (e / jnp.sum(e, axis=-1, keepdims=True)).astype(bf16)
        v = gather_rows(mv, lv_v, gv, s)
        o = matmul(probs, v).reshape(heads, ROWS, cols) * head_mask
        att[r, :] = jnp.sum(o, axis=0)

    chunks = 4
    per_chunk = streams // chunks
    unroll = 4
    for c in range(chunks):

        @pl.loop(0, per_chunk // unroll)
        def _(i):
            for u in range(unroll):
                attend(c * per_chunk + i * unroll + u)

        if c < chunks - 1:
            pump(4 + c)

    def exchange(slot):
        copy = pltpu.make_async_remote_copy(
            src_ref=part.at[slot],
            dst_ref=peer.at[slot],
            send_sem=psend_sem.at[slot],
            recv_sem=precv_sem.at[slot],
            device_id=mdev,
            device_id_type=MESH,
        )
        copy.start()
        return copy

    loads[3].wait()
    complete(3)
    attended = att[...].astype(bf16)
    part[0, :, mine] = matmul(attended, own[3]).astype(bf16)
    part[0, :, other] = matmul(attended, far[3]).astype(bf16)
    first = exchange(0)
    pump(4 + chunks - 1)
    first.wait()

    wide = 16 * ROWS

    @pl.loop(0, total // wide)
    def _(i):
        r = pl.ds(pl.multiple_of(i * wide, wide), wide)
        a = part[0, r, :].astype(f32) + peer[0, r, :].astype(f32)
        a3 = a.reshape(wide // ROWS, ROWS, width)
        row = lax.broadcasted_iota(jnp.int32, a3.shape, 1)
        memory = jnp.sum(jnp.where(row == frames, a3, 0.0), axis=1)
        s = pl.ds(pl.multiple_of(i * 16, 16), 16)
        mnext_ref[s, :] = jnp.tanh(memory).astype(bf16)
        h = x_ref[r, :].astype(f32) + a
        hid[r, :] = h
        rows_v[r, :] = normalize(h).astype(bf16)

    ahead = 4 + chunks
    for j in range(n_ff):
        b = 4 + 2 * j
        pump(ahead)
        ahead += 1
        loads[b].wait()
        complete(b)
        up = matmul(rows_v[:, mine], own[b]) + matmul(rows_v[:, other], far[b])
        hbuf[...] = jax.nn.gelu(up, approximate=True).astype(bf16)
        if ahead <= n_blocks:
            pump(ahead)
            ahead += 1
        loads[b + 1].wait()
        complete(b + 1)
        near = matmul(hbuf[...], own[b + 1])
        away = matmul(hbuf[...], far[b + 1])
        if j == 0:
            dacc[:, mine] = near
            dacc[:, other] = away
        else:
            near = dacc[:, mine] + near
            away = dacc[:, other] + away
            if j < n_ff - 1:
                dacc[:, mine] = near
                dacc[:, other] = away
            else:
                part[1, :, mine] = near.astype(bf16)
                part[1, :, other] = away.astype(bf16)

    second = exchange(1)
    second.wait()

    @pl.loop(0, total // tile)
    def _(i):
        r = pl.ds(pl.multiple_of(i * tile, tile), tile)
        y = hid[r, :] + (part[1, r, :].astype(f32) + peer[1, r, :].astype(f32))
        out_ref[r, :] = (normalize(y) * gain_ref[...]).astype(bf16)

    for copy in sends:
        copy.wait_send()


def shards(
    features,
    memory_bank,
    memory_fill,
    left_keys,
    left_values,
    left_length,
    w_query,
    w_key,
    w_value,
    w_out,
    w_up,
    w_down,
    out_gain,
):
    frames, width_dev, all_streams = features.shape
    streams, mem_slots, width = memory_bank.shape
    left_slots = left_keys.shape[1]
    depth, cols = w_query.shape
    n_ff = w_up.shape[1] // cols
    n_blocks = 4 + 2 * n_ff
    total = streams * ROWS
    n_dp = lax.axis_size("dp")
    n_fsdp = lax.axis_size("fsdp")
    flattened = features.reshape(frames * width_dev, all_streams)
    arrived = lax.all_to_all(flattened, ("dp", "fsdp"), split_axis=1, concat_axis=0, tiled=True)
    arrived = arrived.reshape(n_dp * n_fsdp, frames, width_dev, streams)
    inputs = jnp.transpose(arrived, (3, 1, 0, 2)).reshape(streams, frames, width)
    x = jnp.pad(inputs, ((0, 0), (0, ROWS - frames), (0, 0))).reshape(total, width)
    slot = jnp.arange(KEYS, dtype=jnp.int32)[None, :]
    hidden_mem = (slot < mem_slots) & (slot < (mem_slots - memory_fill)[:, None])
    left_end = mem_slots + left_slots
    hidden_left = (
        (slot >= mem_slots)
        & (slot < left_end)
        & (slot - mem_slots < (left_slots - left_length)[:, None])
    )
    hidden = hidden_mem | hidden_left | (slot >= left_end + frames)
    bias = jnp.where(hidden, -1.0, 0.0).astype(f32)
    vmem = pl.BlockSpec(memory_space=pltpu.VMEM)
    hbm = pl.BlockSpec(memory_space=pl.ANY)
    out, mnext, ck, cv = pl.pallas_call(
        functools.partial(body, frames, mem_slots, left_slots),
        out_shape=(
            jax.ShapeDtypeStruct((total, width), bf16),
            jax.ShapeDtypeStruct((streams, width), bf16),
            jax.ShapeDtypeStruct((total, cols), bf16),
            jax.ShapeDtypeStruct((total, cols), bf16),
        ),
        in_specs=[vmem] * 3 + [hbm] * 9,
        out_specs=(vmem,) * 4,
        scratch_shapes=[
            pltpu.VMEM((n_blocks, depth, cols), bf16),
            pltpu.VMEM((n_blocks, depth, cols), bf16),
            pltpu.VMEM((streams * mem_slots, width), bf16),
            pltpu.VMEM(left_keys.shape, bf16),
            pltpu.VMEM(left_keys.shape, bf16),
            pltpu.VMEM((streams * mem_slots, cols), bf16),
            pltpu.VMEM((streams * mem_slots, cols), bf16),
            pltpu.VMEM((total, cols), f32),
            pltpu.VMEM((total, cols), f32),
            pltpu.VMEM((total, cols), f32),
            pltpu.VMEM((total, width), bf16),
            pltpu.VMEM((total, cols), f32),
            pltpu.VMEM((total, width), f32),
            pltpu.VMEM((total, cols), bf16),
            pltpu.VMEM((total, width), f32),
            pltpu.VMEM((2, total, width), bf16),
            pltpu.VMEM((2, total, width), bf16),
            pltpu.SemaphoreType.DMA((n_blocks, 6)),
            pltpu.SemaphoreType.DMA((n_blocks, 6)),
            pltpu.SemaphoreType.DMA((2,)),
            pltpu.SemaphoreType.DMA((2,)),
            pltpu.SemaphoreType.DMA((n_blocks + 3,)),
        ],
        compiler_params=pltpu.CompilerParams(
            collective_id=0, has_side_effects=True, vmem_limit_bytes=60 * 1024 * 1024
        ),
    )(
        x,
        bias,
        out_gain.reshape(1, width),
        memory_bank.reshape(streams * mem_slots, width),
        left_keys,
        left_values,
        w_query,
        w_key,
        w_value,
        w_out,
        w_up,
        w_down,
    )
    layer_out = out.reshape(streams, ROWS, width)[:, :frames]
    center_keys = ck.reshape(streams, ROWS, cols)[:, :GROUP]
    center_values = cv.reshape(streams, ROWS, cols)[:, :GROUP]
    return (layer_out, mnext, center_keys, center_values)


def solution(mesh):
    in_specs = (
        P(None, ("dp", "fsdp"), None),
        P(("dp", "fsdp"), None, None),
        P(("dp", "fsdp")),
        P(("dp", "fsdp"), None, "mp"),
        P(("dp", "fsdp"), None, "mp"),
        P(("dp", "fsdp")),
        P("fsdp", "mp"),
        P("fsdp", "mp"),
        P("fsdp", "mp"),
        P("mp", "fsdp"),
        P("fsdp", "mp"),
        P("mp", "fsdp"),
        P(),
    )
    out_specs = (
        P(("dp", "fsdp"), None, None),
        P(("dp", "fsdp"), None),
        P(("dp", "fsdp"), None, "mp"),
        P(("dp", "fsdp"), None, "mp"),
    )
    return jax.shard_map(shards, mesh=mesh, in_specs=in_specs, out_specs=out_specs, check_vma=False)
```

```python
import functools

import jax
import jax.numpy as jnp
from jax import lax
from jax.experimental import pallas as pl
from jax.experimental.pallas import tpu as pltpu
from jax.sharding import PartitionSpec as P

HD = 64
GROUP = 4
ROWS = 8
KEYS = 128

epsilon = 1e-05
masked_score = -1e30
MESH = pl.DeviceIdType.MESH
bf16 = jnp.bfloat16
f32 = jnp.float32


def normalize(values):
    average = jnp.mean(values, axis=-1, keepdims=True)
    centred = values - average
    variance = jnp.mean(centred * centred, axis=-1, keepdims=True)
    return centred * lax.rsqrt(variance + epsilon)


def matmul(left, right):
    return jnp.dot(left, right, preferred_element_type=f32)


def body(
    frames,
    mem_slots,
    left_slots,
    packed,
    f_ref,
    fill_ref,
    length_ref,
    gain_ref,
    mem_hbm,
    lk_hbm,
    lv_hbm,
    wq_hbm,
    wk_hbm,
    wv_hbm,
    wo_hbm,
    wu_hbm,
    wd_hbm,
    out_ref,
    mnext_ref,
    ck_ref,
    cv_ref,
    x_ref,
    outbox,
    inbox,
    far,
    own,
    mem_v,
    lk_v,
    lv_v,
    mk,
    mv,
    gk,
    gv,
    qs,
    rows_v,
    att,
    hid,
    hbuf,
    dacc,
    part,
    peer,
    send_sem,
    recv_sem,
    psend_sem,
    precv_sem,
    load_sem,
    fsend_sem,
    frecv_sem,
):
    d = lax.axis_index("dp")
    m = lax.axis_index("mp")
    f = lax.axis_index("fsdp")
    total, width = x_ref.shape
    streams = total // ROWS
    n_blocks, depth, cols = far.shape
    n_ff = (n_blocks - 4) // 2
    quarter = depth // 4
    c1 = quarter // 4
    c2 = (quarter - c1) // 2
    ybit = lax.rem(d, 2)
    zbit = lax.rem(lax.div(d, 2), 2)
    p = lax.rem(d, 4)
    py = p + 1 - 2 * ybit
    pz = p + 2 - 4 * zbit
    pd = 3 - p
    xdev = (d, m, 1 - f)
    ydev = (d + 1 - 2 * ybit, m, f)
    zdev = (d + 2 - 4 * zbit, m, f)
    mdev = (d, 1 - m, f)

    def own_hbm(b, start, size):
        r = pl.ds(pl.multiple_of(start, 16), size)
        if b < 4:
            return (wk_hbm, wv_hbm, wq_hbm, wo_hbm)[b].at[r, :]
        j = (b - 4) // 2
        if b % 2 == 0:
            return wu_hbm.at[r, pl.ds(j * cols, cols)]
        return wd_hbm.at[pl.ds(pl.multiple_of(start + j * depth, 16), size), :]

    def piece(b, start, size):
        return far.at[b, pl.ds(pl.multiple_of(start, 16), size), :]

    sends = []

    def send(src, b, start, size, dev, kind):
        copy = pltpu.make_async_remote_copy(
            src_ref=src,
            dst_ref=piece(b, start, size),
            send_sem=send_sem.at[b, kind],
            recv_sem=recv_sem.at[b, kind],
            device_id=dev,
            device_id_type=MESH,
        )
        copy.start()
        sends.append(copy)

    def arrived(b, start, size, kind):
        ref = piece(b, start, size)
        pltpu.make_async_remote_copy(
            src_ref=ref,
            dst_ref=ref,
            send_sem=send_sem.at[b, kind],
            recv_sem=recv_sem.at[b, kind],
            device_id=xdev,
            device_id_type=MESH,
        ).wait_recv()

    def load(src, dst, i):
        copy = pltpu.make_async_copy(src, dst, load_sem.at[i])
        copy.start()
        return copy

    peers = inbox.shape[0] if packed else 0
    n_fsdp = lax.axis_size("fsdp")
    me = d * n_fsdp + f

    def place(offset):
        return lax.rem(me + offset, peers)

    def device_of(index):
        return (lax.div(index, n_fsdp), m, lax.rem(index, n_fsdp))

    barrier = pltpu.get_barrier_semaphore()
    greeted = [device_of(place(o)) for o in range(1, peers)] if packed else [xdev, ydev, zdev]
    greeted.append(mdev)
    for dev in greeted:
        pl.semaphore_signal(barrier, inc=1, device_id=dev, device_id_type=MESH)

    if packed:
        pairs = outbox.shape[1]
        for k in range(pairs):
            low = f_ref[2 * k].astype(f32)
            high = f_ref[min(2 * k + 1, frames - 1)].astype(f32)
            turned = jnp.concatenate([low, high], axis=0).T.astype(bf16)
            outbox[:, k] = turned.reshape(peers, streams, turned.shape[1])

    pl.semaphore_wait(barrier, len(greeted))

    fsends = []
    for o in range(1, peers):
        copy = pltpu.make_async_remote_copy(
            src_ref=outbox.at[place(o)],
            dst_ref=inbox.at[me],
            send_sem=fsend_sem.at[o],
            recv_sem=frecv_sem.at[o],
            device_id=device_of(place(o)),
            device_id_type=MESH,
        )
        copy.start()
        fsends.append(copy)

    def send_own(b):
        if b >= n_blocks:
            return
        send(own_hbm(b, p * quarter, quarter), b, p * quarter, quarter, xdev, 0)
        send(own_hbm(b, pd * quarter, c1), b, pd * quarter, c1, xdev, 1)

    lead = 3
    for b in range(lead):
        send_own(b)

    loads = [load(own_hbm(b, 0, depth), own.at[b], b) for b in range(n_blocks)]
    mem_load = load(mem_hbm, mem_v, n_blocks)
    lk_load = load(lk_hbm, lk_v, n_blocks + 1)
    lv_load = load(lv_hbm, lv_v, n_blocks + 2)

    def pass_quarter(b):
        if b >= n_blocks:
            return
        arrived(b, p * quarter, quarter, 0)
        send_own(b + lead)
        src = piece(b, p * quarter, quarter)
        send(src, b, p * quarter, quarter, ydev, 2)
        send(src, b, p * quarter, quarter, zdev, 3)

    def pass_diagonal(b):
        if b >= n_blocks:
            return
        at_y = pz * quarter + c1
        arrived(b, pz * quarter, quarter, 3)
        send(piece(b, at_y, c2), b, at_y, c2, ydev, 4)
        at_z = py * quarter + c1 + c2
        arrived(b, py * quarter, quarter, 2)
        send(piece(b, at_z, c2), b, at_z, c2, zdev, 5)

    def complete(b):
        arrived(b, pd * quarter, c1, 1)
        arrived(b, pd * quarter + c1, c2, 4)
        arrived(b, pd * quarter + c1 + c2, c2, 5)

    def pump(b):
        pass_quarter(b)
        pass_diagonal(b - 1)

    mine = pl.ds(pl.multiple_of(f * depth, 128), depth)
    other = pl.ds(pl.multiple_of((1 - f) * depth, 128), depth)
    tile = 64

    if packed:
        inbox[pl.ds(me, 1)] = outbox[pl.ds(me, 1)]
        for o in range(1, peers):
            ref = inbox.at[lax.rem(me + peers - o, peers)]
            pltpu.make_async_remote_copy(
                src_ref=ref,
                dst_ref=ref,
                send_sem=fsend_sem.at[o],
                recv_sem=frecv_sem.at[o],
                device_id=xdev,
                device_id_type=MESH,
            ).wait_recv()
        half = inbox.shape[3] // 2
        parts = []
        for t in range(frames):
            k, side = t // 2, t % 2
            lanes = slice(side * half, side * half + half)
            parts.append(
                jnp.concatenate([inbox[i, k][:, lanes] for i in range(peers)], axis=1)
            )
        major = jnp.concatenate(parts, axis=0)
    else:
        major = f_ref[...]
    count = frames * streams
    r_id = lax.broadcasted_iota(jnp.int32, (total, count), 0)
    c_id = lax.broadcasted_iota(jnp.int32, (total, count), 1)
    frame_id = r_id % ROWS
    target = jnp.where(frame_id < frames, frame_id * streams + r_id // ROWS, -1)
    x_ref[...] = matmul(jnp.where(target == c_id, 1.0, 0.0).astype(bf16), major).astype(bf16)

    @pl.loop(0, total // tile)
    def _(i):
        r = pl.ds(pl.multiple_of(i * tile, tile), tile)
        n = normalize(x_ref[r, :].astype(f32)).astype(bf16).astype(f32)
        n3 = n.reshape(tile // ROWS, ROWS, width)
        row = lax.broadcasted_iota(jnp.int32, n3.shape, 1)
        mean = jnp.sum(jnp.where(row < GROUP, n3, 0.0), axis=1, keepdims=True) * (1.0 / GROUP)
        n3 = jnp.where(row == frames, jnp.broadcast_to(mean, n3.shape), n3)
        rows_v[r, :] = n3.reshape(tile, width).astype(bf16)

    mem_load.wait()
    pass_quarter(0)
    pump(1)

    def project(b):
        loads[b].wait()
        complete(b)
        sums = matmul(rows_v[:, mine], own[b]) + matmul(rows_v[:, other], far[b])
        return sums.astype(bf16)

    def project_memory(b, target):
        step = 256

        @pl.loop(0, mem_v.shape[0] // step)
        def _(i):
            r = pl.ds(pl.multiple_of(i * step, step), step)
            sums = matmul(mem_v[r, mine], own[b]) + matmul(mem_v[r, other], far[b])
            target[r, :] = sums.astype(bf16)

    keys = project(0)
    ck_ref[...] = keys
    gk[...] = keys.astype(f32)
    project_memory(0, mk)
    pump(2)
    vals = project(1)
    cv_ref[...] = vals
    gv[...] = vals.astype(f32)
    project_memory(1, mv)
    pump(3)
    qs[...] = project(2).astype(f32)
    lk_load.wait()
    lv_load.wait()

    heads = cols // HD
    lanes3 = lax.broadcasted_iota(jnp.int32, (heads, ROWS, cols), 2)
    head3 = lax.broadcasted_iota(jnp.int32, (heads, ROWS, cols), 0)
    head_mask = jnp.where(lanes3 // HD == head3, 1.0, 0.0).astype(f32)
    row2 = lax.broadcasted_iota(jnp.int32, (heads * ROWS, KEYS), 0)
    lane2 = lax.broadcasted_iota(jnp.int32, (heads * ROWS, KEYS), 1)
    excluded = jnp.where((row2 % ROWS == frames) & (lane2 < mem_slots), -1.0, 0.0).astype(f32)
    lane1 = lax.broadcasted_iota(jnp.int32, (1, KEYS), 1)
    left_end = mem_slots + left_slots
    pad8 = jnp.zeros((16 - ROWS, cols), f32)
    pad = jnp.zeros((KEYS - mem_slots - left_slots - 16, cols), bf16)
    scale = HD ** (-0.5)

    def gather_rows(mem_part, left_part, group_part, s):
        return jnp.concatenate(
            [
                mem_part[pl.ds(pl.multiple_of(s * mem_slots, mem_slots), mem_slots), :],
                left_part[s],
                jnp.concatenate(
                    [group_part[pl.ds(pl.multiple_of(s * ROWS, ROWS), ROWS), :], pad8], axis=0
                ).astype(bf16),
                pad,
            ],
            axis=0,
        )

    def attend(s):
        r = pl.ds(pl.multiple_of(s * ROWS, ROWS), ROWS)
        spread = (qs[r, :][None] * head_mask).reshape(heads * ROWS, cols).astype(bf16)
        k = gather_rows(mk, lk_v, gk, s)
        scores = (
            lax.dot_general(spread, k, (((1,), (1,)), ((), ())), preferred_element_type=f32) * scale
        )
        first_mem = mem_slots - fill_ref[s]
        first_left = left_end - length_ref[s]
        first = jnp.where(lane1 < mem_slots, first_mem, first_left)
        first = jnp.where(lane1 < left_end, first, 0)
        hide1 = (lane1 < first) | (lane1 >= left_end + frames)
        hide = jnp.where(hide1, -1.0, 0.0) + excluded
        scores = jnp.where(hide < 0.0, masked_score, scores)
        top = jnp.max(scores, axis=-1, keepdims=True)
        e = jnp.exp(scores - top)
        probs = (e / jnp.sum(e, axis=-1, keepdims=True)).astype(bf16)
        v = gather_rows(mv, lv_v, gv, s)
        o = matmul(probs, v).reshape(heads, ROWS, cols) * head_mask
        att[r, :] = jnp.sum(o, axis=0)

    chunks = 4
    per_chunk = streams // chunks
    unroll = 4
    for c in range(chunks):

        @pl.loop(0, per_chunk // unroll)
        def _(i):
            for u in range(unroll):
                attend(c * per_chunk + i * unroll + u)

        if c < chunks - 1:
            pump(4 + c)

    def exchange(slot):
        copy = pltpu.make_async_remote_copy(
            src_ref=part.at[slot],
            dst_ref=peer.at[slot],
            send_sem=psend_sem.at[slot],
            recv_sem=precv_sem.at[slot],
            device_id=mdev,
            device_id_type=MESH,
        )
        copy.start()
        return copy

    loads[3].wait()
    complete(3)
    attended = att[...].astype(bf16)
    part[0, :, mine] = matmul(attended, own[3]).astype(bf16)
    part[0, :, other] = matmul(attended, far[3]).astype(bf16)
    first = exchange(0)
    pump(4 + chunks - 1)
    first.wait()

    wide = 16 * ROWS

    @pl.loop(0, total // wide)
    def _(i):
        r = pl.ds(pl.multiple_of(i * wide, wide), wide)
        a = part[0, r, :].astype(f32) + peer[0, r, :].astype(f32)
        a3 = a.reshape(wide // ROWS, ROWS, width)
        row = lax.broadcasted_iota(jnp.int32, a3.shape, 1)
        memory = jnp.sum(jnp.where(row == frames, a3, 0.0), axis=1)
        s = pl.ds(pl.multiple_of(i * 16, 16), 16)
        mnext_ref[s, :] = jnp.tanh(memory).astype(bf16)
        h = x_ref[r, :].astype(f32) + a
        hid[r, :] = h
        rows_v[r, :] = normalize(h).astype(bf16)

    ahead = 4 + chunks
    for j in range(n_ff):
        b = 4 + 2 * j
        pump(ahead)
        ahead += 1
        loads[b].wait()
        complete(b)
        up = matmul(rows_v[:, mine], own[b]) + matmul(rows_v[:, other], far[b])
        hbuf[...] = jax.nn.gelu(up, approximate=True).astype(bf16)
        if ahead <= n_blocks:
            pump(ahead)
            ahead += 1
        loads[b + 1].wait()
        complete(b + 1)
        near = matmul(hbuf[...], own[b + 1])
        away = matmul(hbuf[...], far[b + 1])
        if j == 0:
            dacc[:, mine] = near
            dacc[:, other] = away
        else:
            near = dacc[:, mine] + near
            away = dacc[:, other] + away
            if j < n_ff - 1:
                dacc[:, mine] = near
                dacc[:, other] = away
            else:
                part[1, :, mine] = near.astype(bf16)
                part[1, :, other] = away.astype(bf16)

    second = exchange(1)
    second.wait()

    @pl.loop(0, total // tile)
    def _(i):
        r = pl.ds(pl.multiple_of(i * tile, tile), tile)
        y = hid[r, :] + (part[1, r, :].astype(f32) + peer[1, r, :].astype(f32))
        out_ref[r, :] = (normalize(y) * gain_ref[...]).astype(bf16)

    for copy in sends + fsends:
        copy.wait_send()


def finish(frames, rows_ref, mem_ref, keys_ref, vals_ref, out_ref, mnext_ref, ck_ref, cv_ref):
    total, width = rows_ref.shape
    streams = total // ROWS
    count = frames * streams
    r_id = lax.broadcasted_iota(jnp.int32, (count, total), 0)
    c_id = lax.broadcasted_iota(jnp.int32, (count, total), 1)
    pick = (r_id % streams) * ROWS + r_id // streams
    moved = matmul(jnp.where(pick == c_id, 1.0, 0.0).astype(bf16), rows_ref[...])
    out_ref[...] = moved.astype(bf16)
    mnext_ref[...] = mem_ref[...]
    for src, dst in ((keys_ref, ck_ref), (vals_ref, cv_ref)):
        values = src[...].astype(f32).reshape(streams, ROWS, src.shape[1])
        dst[...] = values[:, :GROUP].astype(bf16)


def shards(
    features,
    memory_bank,
    memory_fill,
    left_keys,
    left_values,
    left_length,
    w_query,
    w_key,
    w_value,
    w_out,
    w_up,
    w_down,
    out_gain,
):
    frames, width_dev, all_streams = features.shape
    streams, mem_slots, width = memory_bank.shape
    left_slots = left_keys.shape[1]
    depth, cols = w_query.shape
    n_ff = w_up.shape[1] // cols
    n_blocks = 4 + 2 * n_ff
    total = streams * ROWS
    n_dp = lax.axis_size("dp")
    n_fsdp = lax.axis_size("fsdp")
    peers = n_dp * n_fsdp
    packed = 2 * width_dev == KEYS and streams % 16 == 0
    if packed:
        feed = features
    else:
        flat = features.reshape(frames * width_dev, all_streams)
        got = lax.all_to_all(flat, ("dp", "fsdp"), split_axis=1, concat_axis=0, tiled=True)
        got = got.reshape(peers, frames, width_dev, streams)
        feed = jnp.transpose(got, (1, 3, 0, 2)).reshape(frames * streams, width)
    slots = (peers, (frames + 1) // 2, streams, KEYS) if packed else (1, 1, 16, KEYS)
    vmem = pl.BlockSpec(memory_space=pltpu.VMEM)
    hbm = pl.BlockSpec(memory_space=pl.ANY)
    smem = pl.BlockSpec(memory_space=pltpu.SMEM)
    out, mnext, ck, cv = pl.pallas_call(
        functools.partial(body, frames, mem_slots, left_slots, packed),
        out_shape=(
            jax.ShapeDtypeStruct((total, width), bf16),
            jax.ShapeDtypeStruct((streams, width), bf16),
            jax.ShapeDtypeStruct((total, cols), bf16),
            jax.ShapeDtypeStruct((total, cols), bf16),
        ),
        in_specs=[vmem, smem, smem, vmem] + [hbm] * 9,
        out_specs=(vmem,) * 4,
        scratch_shapes=[
            pltpu.VMEM((total, width), bf16),
            pltpu.VMEM(slots, bf16),
            pltpu.VMEM(slots, bf16),
            pltpu.VMEM((n_blocks, depth, cols), bf16),
            pltpu.VMEM((n_blocks, depth, cols), bf16),
            pltpu.VMEM((streams * mem_slots, width), bf16),
            pltpu.VMEM(left_keys.shape, bf16),
            pltpu.VMEM(left_keys.shape, bf16),
            pltpu.VMEM((streams * mem_slots, cols), bf16),
            pltpu.VMEM((streams * mem_slots, cols), bf16),
            pltpu.VMEM((total, cols), f32),
            pltpu.VMEM((total, cols), f32),
            pltpu.VMEM((total, cols), f32),
            pltpu.VMEM((total, width), bf16),
            pltpu.VMEM((total, cols), f32),
            pltpu.VMEM((total, width), f32),
            pltpu.VMEM((total, cols), bf16),
            pltpu.VMEM((total, width), f32),
            pltpu.VMEM((2, total, width), bf16),
            pltpu.VMEM((2, total, width), bf16),
            pltpu.SemaphoreType.DMA((n_blocks, 6)),
            pltpu.SemaphoreType.DMA((n_blocks, 6)),
            pltpu.SemaphoreType.DMA((2,)),
            pltpu.SemaphoreType.DMA((2,)),
            pltpu.SemaphoreType.DMA((n_blocks + 3,)),
            pltpu.SemaphoreType.DMA((peers,)),
            pltpu.SemaphoreType.DMA((peers,)),
        ],
        compiler_params=pltpu.CompilerParams(
            collective_id=0, has_side_effects=True, vmem_limit_bytes=60 * 1024 * 1024
        ),
    )(
        feed,
        memory_fill,
        left_length,
        out_gain.reshape(1, width),
        memory_bank.reshape(streams * mem_slots, width),
        left_keys,
        left_values,
        w_query,
        w_key,
        w_value,
        w_out,
        w_up,
        w_down,
    )
    layer_out, memory_next, center_keys, center_values = pl.pallas_call(
        functools.partial(finish, frames),
        out_shape=(
            jax.ShapeDtypeStruct((frames * streams, width), bf16),
            jax.ShapeDtypeStruct((streams, width), bf16),
            jax.ShapeDtypeStruct((streams, GROUP, cols), bf16),
            jax.ShapeDtypeStruct((streams, GROUP, cols), bf16),
        ),
        in_specs=[vmem] * 4,
        out_specs=(vmem,) * 4,
    )(out, mnext, ck, cv)
    layer_out = jnp.transpose(layer_out.reshape(frames, streams, width), (1, 0, 2))
    return (layer_out, memory_next, center_keys, center_values)


def solution(mesh):
    in_specs = (
        P(None, ("dp", "fsdp"), None),
        P(("dp", "fsdp"), None, None),
        P(("dp", "fsdp")),
        P(("dp", "fsdp"), None, "mp"),
        P(("dp", "fsdp"), None, "mp"),
        P(("dp", "fsdp")),
        P("fsdp", "mp"),
        P("fsdp", "mp"),
        P("fsdp", "mp"),
        P("mp", "fsdp"),
        P("fsdp", "mp"),
        P("mp", "fsdp"),
        P(),
    )
    out_specs = (
        P(("dp", "fsdp"), None, None),
        P(("dp", "fsdp"), None),
        P(("dp", "fsdp"), None, "mp"),
        P(("dp", "fsdp"), None, "mp"),
    )
    return jax.shard_map(shards, mesh=mesh, in_specs=in_specs, out_specs=out_specs, check_vma=False)
```
